128 devices in a mesh: dp: 16 (over y, x_lo, core), shard: 8 (over z, x_hi).
Axes of the slice: x: 4 (x_hi: 2, x_lo: 2; x = x_hi * 2 + x_lo), y: 4, z: 4, core: 2. Of those that a mesh axis runs over, the one named last changes fastest.
Arguments:
- gradients: bfloat16 [16, 88, 512, 512], P('dp', 'shard'), may hold values from -60 to 60
- owners: int32 [8, 11], P('shard'), may hold values from 0 to 15, as said below
- block_param: int32 [88], replicated, may hold values from 0 to 6, never falling along the last dimension, each value on 1 to 25 neighbouring positions
- left_stat: float32 [32, 8, 512, 512], P('dp', 'shard'), may hold values from -4 to 8, as said below
- right_stat: float32 [32, 8, 512, 512], P('dp', 'shard'), may hold values from -4 to 8, as said below
- moment: float32 [32, 8, 512, 512], P('dp', 'shard'), may hold values from 0.5 to 50
- left_root: bfloat16 [32, 8, 512, 512], P('dp', 'shard'), may hold values from -1 to 3.5, as said below
- right_root: bfloat16 [32, 8, 512, 512], P('dp', 'shard'), may hold values from -1 to 3.5, as said below
Outputs:
- new_left: float32 [32, 8, 512, 512], P('dp', 'shard')
- new_right: float32 [32, 8, 512, 512], P('dp', 'shard')
- new_moment: float32 [32, 8, 512, 512], P('dp', 'shard')
- update: bfloat16 [88, 512, 512], P('shard')
The draws below stay inside these ranges and needn't reach their ends.
Inputs may be any that keep to these rules, and one draw needn't show every extreme that they name: `owners`: in each row, no value occurs more than 2 times, and some value occurs exactly 2 times. `left_stat`: each slot's matrix is symmetric. `right_stat`: each slot's matrix is symmetric. `left_root`: each slot's matrix is symmetric. `right_root`: each slot's matrix is symmetric.
All inputs are finite; a program needn't handle non-finite values.
Results may differ from the reference program's by a relative error of at most 0.0058.
Values may be sent and summed in bfloat16 or wider, within the bound.
A program may use at most 192 MiB of HBM per device.

```python
import math
import jax
import jax.numpy as jnp
import numpy as np
from jax import lax

BLOCK = 512
NBLK = 11
CAP = 2
NPARAM = 7
NBLK_ALL = 88
N_DP = 16
N_SHARD = 8


def draw_gradients(key, part):
    noise_key, scale_key = jax.random.split(jax.random.fold_in(key, 11), 2)
    noise = jax.random.normal(noise_key, (N_DP, NBLK_ALL, BLOCK, BLOCK), jnp.float32)
    scales = jnp.exp(jax.random.uniform(scale_key, (1, NBLK_ALL, 1, 1), jnp.float32, math.log(0.075), math.log(0.75))) / math.sqrt(N_DP)
    values = noise * scales
    return jnp.clip(values, -60.0, 60.0).astype(jnp.bfloat16)


def draw_owners(key, part):

    def one_column(column):
        column_key = jax.random.fold_in(key, 101 + column)
        rank_key, first_key, order_key = jax.random.split(column_key, 3)
        ranks = jax.random.permutation(rank_key, N_DP * CAP).astype(jnp.int32)
        doubled = jax.random.randint(first_key, (), 0, N_DP)
        slot_ids = jnp.arange(N_DP * CAP, dtype=jnp.int32)
        ranks = jnp.where(slot_ids // CAP == doubled, slot_ids % CAP - CAP, ranks)
        ordered = jnp.argsort(ranks, stable=True)
        chosen = (ordered[:NBLK] // CAP).astype(jnp.int32)
        return jax.random.permutation(order_key, chosen)
    return jax.vmap(one_column)(jnp.arange(N_SHARD, dtype=jnp.int32)).astype(jnp.int32)


def symmetric_stat(key):
    noise_key, diag_key = jax.random.split(key)
    noise = jax.random.normal(noise_key, (N_DP * CAP, N_SHARD, BLOCK, BLOCK), jnp.float32)
    diagonal = jnp.exp(jax.random.uniform(diag_key, (N_DP * CAP, N_SHARD, BLOCK, 1), jnp.float32, math.log(0.5), math.log(5.0)))
    symmetric = (noise + jnp.swapaxes(noise, -1, -2)) * 0.2
    values = symmetric + diagonal * jnp.eye(BLOCK, dtype=jnp.float32)
    return jnp.clip(values, -4.0, 8.0)


def symmetric_root(key):
    noise_key, diag_key = jax.random.split(key)
    noise = jax.random.normal(noise_key, (N_DP * CAP, N_SHARD, BLOCK, BLOCK), jnp.float32)
    diagonal = jax.random.uniform(diag_key, (N_DP * CAP, N_SHARD, BLOCK, 1), jnp.float32, 1.5, 3.0)
    symmetric = (noise + jnp.swapaxes(noise, -1, -2)) * (0.5 / math.sqrt(2.0 * BLOCK))
    values = symmetric + diagonal * jnp.eye(BLOCK, dtype=jnp.float32)
    return jnp.clip(values, -1.0, 3.5).astype(jnp.bfloat16)


def draw_left_stat(key, part):
    return symmetric_stat(jax.random.fold_in(key, 21))


def draw_right_stat(key, part):
    return symmetric_stat(jax.random.fold_in(key, 22))


def draw_left_root(key, part):
    return symmetric_root(jax.random.fold_in(key, 31))


def draw_right_root(key, part):
    return symmetric_root(jax.random.fold_in(key, 32))


def shard_levels(stream_key, dims, shards, low, top_value):
    def one(axis_at, blocks):
        steps = jax.random.uniform(jax.random.fold_in(jax.random.fold_in(stream_key, 6), axis_at), (blocks,), jnp.float32, low / len(shards), top_value / len(shards))
        return jnp.repeat(jnp.exp(steps), dims[axis_at] // blocks).reshape((-1,) + (1,) * (len(dims) - axis_at - 1))

    factor_of = one(*shards[0])
    for cut in shards[1:]:
        factor_of = factor_of * one(*cut)
    return factor_of


def profile(amount, total, most, slope):
    portions = [(1 << 20) // math.isqrt(rank ** slope) + 1 for rank in range(2, amount + 1)]
    spare, holding = total - most - (amount - 1), [1] * (amount - 1)
    while spare > 0:
        movable = [i for i in range(amount - 1) if holding[i] < most]
        whole, left = sum([portions[i] for i in movable]), spare
        for i in movable:
            addition = min(most - holding[i], max(1, left * portions[i] // whole), spare)
            holding[i] = holding[i] + addition
            spare = spare - addition
    return np.array([most] + holding)


def uneven_parts(rng, count, total, bound, skew):
    if count == 2:
        one = jax.random.randint(rng, (), max(1, total - bound), min(bound, total - 1) + 1)
        return jnp.stack([one, total - one])
    sizes = jnp.asarray(profile(count, total, bound, skew), jnp.int32)
    pairs = (count - 1) // 2
    giver, taker = sizes[1:1 + 2 * pairs:2], sizes[2:2 + 2 * pairs:2]
    slack = jnp.minimum(giver - 1, bound - taker)
    passed = jax.random.randint(jax.random.fold_in(rng, 1), (pairs,), 0, 1 << 20) % (slack + 1)
    sizes = sizes.at[1:1 + 2 * pairs:2].set(giver - passed).at[2:2 + 2 * pairs:2].set(taker + passed)
    return sizes[jax.random.permutation(jax.random.fold_in(rng, 2), count)]


def setup_inputs(seed: int = 0) -> dict:
    streams_of = jax.random.split(jax.random.key(seed), 9)
    return {
        "gradients": draw_gradients(jax.random.fold_in(streams_of[8], 71), 0),
        "owners": draw_owners(jax.random.fold_in(streams_of[8], 71), 0),
        "block_param": jnp.searchsorted(jnp.cumsum(uneven_parts(streams_of[2], NPARAM, NBLK_ALL, 2 * NBLK_ALL // NPARAM, 0)), jnp.arange(NBLK_ALL), side="right").astype(jnp.int32),
        "left_stat": draw_left_stat(jax.random.fold_in(streams_of[8], 71), 0),
        "right_stat": draw_right_stat(jax.random.fold_in(streams_of[8], 71), 0),
        "moment": jnp.clip(jnp.exp(math.log(50.0) - 4.6051702 * jax.random.uniform(streams_of[5], (N_DP * CAP, N_SHARD, BLOCK, BLOCK), jnp.float32) ** shard_levels(streams_of[5], (N_DP * CAP, N_SHARD, BLOCK, BLOCK), ((0, 16), (1, 8)), -0.2, 0.2)), 0.5, 50.0),
        "left_root": draw_left_root(jax.random.fold_in(streams_of[8], 71), 0),
        "right_root": draw_right_root(jax.random.fold_in(streams_of[8], 71), 0),
    }


decay_rate = 0.95
tiny_value = 1e-06

def slot_numbers(owners):
    counter = jnp.arange(owners.shape[1], dtype=jnp.int32)
    same_owner = owners[:, :, None] == owners[:, None, :]
    earlier = counter[None, :] < counter[:, None]
    return lax.optimization_barrier(jnp.sum(jnp.where(same_owner & earlier[None], 1, 0), axis=2)).astype(jnp.int32)

def block_products(operands):
    gradient, left_factor, right_factor = operands
    left_gram = jnp.dot(gradient, gradient.T, precision=lax.Precision.HIGHEST)
    right_gram = jnp.dot(gradient.T, gradient, precision=lax.Precision.HIGHEST)
    left_half = jnp.dot(left_factor, gradient.astype(jnp.bfloat16), preferred_element_type=jnp.float32).astype(jnp.bfloat16)
    direction = jnp.dot(left_half, right_factor, preferred_element_type=jnp.float32)
    return (left_gram, right_gram, direction)

def reference(gradients, owners, block_param, left_stat, right_stat, moment, left_root, right_root):
    summed = lax.optimization_barrier(jnp.sum(gradients, axis=0, dtype=jnp.float32))
    places = owners * CAP + slot_numbers(owners)
    column_ids = jnp.arange(N_SHARD, dtype=jnp.int32)
    left_roots = left_root[places, column_ids[:, None]].reshape(NBLK_ALL, BLOCK, BLOCK)
    right_roots = right_root[places, column_ids[:, None]].reshape(NBLK_ALL, BLOCK, BLOCK)
    left_gram, right_gram, direction = lax.map(block_products, (summed, left_roots, right_roots))
    slot_ids = jnp.arange(N_DP * CAP, dtype=jnp.int32)
    matches = places[:, None, :] == slot_ids[None, :, None]
    is_live = jnp.any(matches, axis=2)
    block_index = lax.optimization_barrier(jnp.sum(jnp.where(matches, jnp.arange(NBLK, dtype=jnp.int32)[None, None, :], 0), axis=2)).astype(jnp.int32)
    flat_index = (column_ids[:, None] * NBLK + block_index).T
    live_mask = is_live.T[:, :, None, None]
    held = jnp.where(live_mask, summed[flat_index], 0.0)
    new_left = decay_rate * left_stat + (1.0 - decay_rate) * jnp.where(live_mask, left_gram[flat_index], 0.0)
    new_right = decay_rate * right_stat + (1.0 - decay_rate) * jnp.where(live_mask, right_gram[flat_index], 0.0)
    new_moment = decay_rate * moment + (1.0 - decay_rate) * held * held
    adam_step = held / (jnp.sqrt(new_moment) + tiny_value)
    adam_squares = lax.optimization_barrier(jnp.sum(adam_step * adam_step, axis=(2, 3)))
    param_ids = jnp.arange(NPARAM, dtype=jnp.int32)
    slot_member = (block_param[flat_index][:, :, None] == param_ids[None, None, :]) & is_live.T[:, :, None]
    adam_norm = lax.optimization_barrier(jnp.sum(jnp.where(slot_member, adam_squares[:, :, None], 0.0), axis=(0, 1)))
    block_member = block_param[:, None] == param_ids[None, :]
    direction_squares = lax.optimization_barrier(jnp.sum(direction * direction, axis=(1, 2)))
    direction_norm = lax.optimization_barrier(jnp.sum(jnp.where(block_member, direction_squares[:, None], 0.0), axis=0))
    graft_ratio = jnp.sqrt((adam_norm + tiny_value) / (direction_norm + tiny_value))
    block_ratio = lax.optimization_barrier(jnp.sum(jnp.where(block_member, graft_ratio[None, :], 0.0), axis=1))
    update = (block_ratio[:, None, None] * direction).astype(jnp.bfloat16)
    return (new_left, new_right, new_moment, update)
```

```python
import functools

import jax
import jax.numpy as jnp
from jax import lax
from jax.experimental import pallas as pl
from jax.experimental.pallas import tpu as pltpu
from jax.sharding import PartitionSpec as P

NPARAM = 7
DECAY = 0.95
TINY = 1e-06
NY, NX, NC = 4, 2, 2
BF = jnp.bfloat16
F32 = jnp.float32


def position():
    d = lax.axis_index("dp")
    return d // 4, (d // 2) % 2, d % 2


def flat(y, x, c):
    return (y % NY) * 4 + (x % NX) * 2 + c % NC


OFFSETS = [
    (dy, dx, dc)
    for dy in (2, 1, 3, 0)
    for dx in (1, 0)
    for dc in (0, 1)
    if (dy, dx, dc) != (0, 0, 0)
]


class Copies:
    def __init__(self, send, recv):
        self.send, self.recv, self.count, self.all = send, recv, 0, []

    def start(self, src, dst, where):
        i = self.count
        self.count += 1
        copy = pltpu.make_async_remote_copy(
            src_ref=src,
            dst_ref=dst,
            send_sem=self.send.at[i],
            recv_sem=self.recv.at[i],
            device_id=where,
            device_id_type=pl.DeviceIdType.MESH,
        )
        copy.start()
        self.all.append(copy)
        return copy

    def finish(self):
        for copy in self.all:
            copy.wait_send()


def add_blocks(count, out, first, second):
    def body(b, carry):
        out[b] = first[b] + second[b]
        return carry

    lax.fori_loop(0, count, body, 0)


def add_many(count, out, *terms):
    def body(b, carry):
        total = terms[0][b].astype(F32)
        for term in terms[1:]:
            total = total + term[b].astype(F32)
        out[b] = total.astype(BF)
        return carry

    lax.fori_loop(0, count, body, 0)


def reduce_kernel(
    nblk, na_blk, source_ref, grad_ref, held_ref, loc, rem, far_a, mid_b, near_a, mid_a,
    far_b, near_b, share, stage, local_sem, send_sem, recv_sem,
):
    y, x, c = position()
    nb_blk = nblk - na_blk
    rows = share.shape[1]
    half = rows // 2
    ox, oc = 1 - x, 1 - c
    up, down, across = (y + 1) % NY, (y + 3) % NY, (y + 2) % NY
    A = pl.ds(0, na_blk)
    B = pl.ds(na_blk, nb_blk)
    H = (pl.ds(0, half), pl.ds(half, half))

    def gpart(which, core):
        return [
            grad_ref.at[A, core, across],
            grad_ref.at[B, core, :, ox],
            grad_ref.at[A, core, up],
            grad_ref.at[A, core, down],
            grad_ref.at[B, core, :, x],
            grad_ref.at[A, core, y],
        ][which]

    def vpart(buf, which):
        return [
            buf.at[A, across],
            buf.at[B, :, ox],
            buf.at[A, up],
            buf.at[A, down],
            buf.at[B, :, x],
            buf.at[A, y],
        ][which]

    loads = []
    for i in range(6):
        load = pltpu.make_async_copy(gpart(i, c), vpart(loc, i), local_sem.at[i])
        load.start()
        loads.append(load)

    barrier = pltpu.get_barrier_semaphore()
    for dy, dx, dc in OFFSETS:
        pl.semaphore_signal(
            barrier, inc=1, device_id={"dp": flat(y + dy, x + dx, c + dc)},
            device_id_type=pl.DeviceIdType.MESH,
        )
    pl.semaphore_wait(barrier, len(OFFSETS))

    to_core = {"dp": flat(y, x, oc)}
    to_x = {"dp": flat(y, ox, c)}
    to_up = {"dp": flat(up, x, c)}
    to_down = {"dp": flat(down, x, c)}
    copies = Copies(send_sem, recv_sem)
    pair = [copies.start(gpart(i, oc), vpart(rem, i), to_core) for i in range(6)]

    def pair_sum(i):
        loads[i].wait()
        pair[i].wait_recv()
        mine, other = vpart(loc, i), vpart(rem, i)
        inner = mine.shape[1]
        for j in range(inner):
            add_blocks(
                mine.shape[0], mine.at[:, j], mine.at[:, j], other.at[:, j]
            )

    pair_sum(0)
    fa = [
        copies.start(loc.at[A, across, 0], far_a.at[0], to_up),
        copies.start(loc.at[A, across, 1], far_a.at[1], to_down),
    ]
    pair_sum(1)
    mb = [
        copies.start(loc.at[B, chunk, ox], mid_b.at[:, chunk], to_x)
        for chunk in (across, up, down, y)
    ]
    pair_sum(2)
    n_a = {(0, 1): copies.start(loc.at[A, up, 1], near_a.at[0, 1], to_up)}
    pair_sum(3)
    n_a[1, 0] = copies.start(loc.at[A, down, 0], near_a.at[1, 0], to_down)
    pair_sum(4)
    pair_sum(5)

    fa[0].wait_recv()
    add_blocks(na_blk, loc.at[A, up, 0], loc.at[A, up, 0], far_a.at[0])
    n_a[0, 0] = copies.start(loc.at[A, up, 0], near_a.at[0, 0], to_up)
    fa[1].wait_recv()
    add_blocks(na_blk, loc.at[A, down, 1], loc.at[A, down, 1], far_a.at[1])
    n_a[1, 1] = copies.start(loc.at[A, down, 1], near_a.at[1, 1], to_down)

    def middle(i, chunk):
        mb[i].wait_recv()
        add_blocks(nb_blk, loc.at[B, chunk, x], loc.at[B, chunk, x], mid_b.at[:, chunk])

    middle(0, across)
    fb = [
        copies.start(loc.at[B, across, x, H[0]], far_b.at[0], to_up),
        copies.start(loc.at[B, across, x, H[1]], far_b.at[1], to_down),
    ]
    middle(1, up)
    n_b = {(0, 1): copies.start(loc.at[B, up, x, H[1]], near_b.at[0, 1], to_up)}
    middle(2, down)
    n_b[1, 0] = copies.start(loc.at[B, down, x, H[0]], near_b.at[1, 0], to_down)

    for key in ((0, 1), (1, 0), (0, 0), (1, 1)):
        n_a[key].wait_recv()
    add_many(na_blk, loc.at[A, y, ox], loc.at[A, y, ox], near_a.at[0, ox], near_a.at[1, ox])
    ma = copies.start(loc.at[A, y, ox], mid_a, to_x)

    fb[0].wait_recv()
    add_blocks(nb_blk, loc.at[B, up, x, H[0]], loc.at[B, up, x, H[0]], far_b.at[0])
    n_b[0, 0] = copies.start(loc.at[B, up, x, H[0]], near_b.at[0, 0], to_up)
    fb[1].wait_recv()
    add_blocks(nb_blk, loc.at[B, down, x, H[1]], loc.at[B, down, x, H[1]], far_b.at[1])
    n_b[1, 1] = copies.start(loc.at[B, down, x, H[1]], near_b.at[1, 1], to_down)

    share[nblk] = jnp.zeros(share.shape[1:], BF)
    ma.wait_recv()
    add_many(
        na_blk, share.at[A], loc.at[A, y, x], near_a.at[0, x], near_a.at[1, x], mid_a
    )
    mb[3].wait_recv()
    for key in ((0, 1), (1, 0), (0, 0), (1, 1)):
        n_b[key].wait_recv()
    for h in range(2):
        add_many(
            nb_blk, share.at[B, H[h]], loc.at[B, y, x, H[h]], mid_b.at[:, y, H[h]],
            near_b.at[0, h], near_b.at[1, h],
        )

    sent = []
    for k, (dy, dx, dc) in enumerate(OFFSETS):
        q = flat(y + dy, x + dx, c + dc)
        for j in range(2):
            stage[k, j] = share[source_ref[q * 2 + j]]
        sent.append(copies.start(stage.at[k], held_ref.at[:, c, y, x], {"dp": q}))
    mine = flat(y, x, c)
    for j in range(2):
        held_ref[j, c, y, x] = share[source_ref[mine * 2 + j]]
    for copy in sent:
        copy.wait_recv()
    copies.finish()


def reduce_to_owners(gradients, source):
    nblk, block, width = gradients.shape
    rows = block // (NY * NX * NC)
    na_blk = (nblk + 1) // 2
    nb_blk = nblk - na_blk
    n_copies = 6 + 2 + 4 + 4 + 2 + 4 + 1 + len(OFFSETS)
    held = pl.pallas_call(
        functools.partial(reduce_kernel, nblk, na_blk),
        out_shape=jax.ShapeDtypeStruct((2, NC, NY, NX, rows, width), BF),
        in_specs=[
            pl.BlockSpec(memory_space=pltpu.SMEM),
            pl.BlockSpec(memory_space=pl.ANY),
        ],
        out_specs=pl.BlockSpec(memory_space=pltpu.VMEM),
        scratch_shapes=[
            pltpu.VMEM((nblk, NY, NX, rows, width), BF),
            pltpu.VMEM((nblk, NY, NX, rows, width), BF),
            pltpu.VMEM((2, na_blk, rows, width), BF),
            pltpu.VMEM((nb_blk, NY, rows, width), BF),
            pltpu.VMEM((2, 2, na_blk, rows, width), BF),
            pltpu.VMEM((na_blk, rows, width), BF),
            pltpu.VMEM((2, nb_blk, rows // 2, width), BF),
            pltpu.VMEM((2, 2, nb_blk, rows // 2, width), BF),
            pltpu.VMEM((nblk + 1, rows, width), BF),
            pltpu.VMEM((len(OFFSETS), 2, rows, width), BF),
            pltpu.SemaphoreType.DMA((6,)),
            pltpu.SemaphoreType.DMA((n_copies,)),
            pltpu.SemaphoreType.DMA((n_copies,)),
        ],
        compiler_params=pltpu.CompilerParams(collective_id=0, has_side_effects=True),
        name="reduce_to_owners",
    )(source, gradients.reshape(nblk, NC, NY, NX, rows, width))
    return held.reshape(2, block, width)


def slot_kernel(
    param_ref, held_ref, lroot_ref, rroot_ref, lstat_ref, rstat_ref, moment_ref,
    nl_ref, nr_ref, nm_ref, dir_ref, norm_ref, acc,
):
    s, r = pl.program_id(0), pl.program_id(1)
    step = lstat_ref.shape[1]
    at = pl.multiple_of(r * step, step)
    held = held_ref[0]
    part = held_ref[0, pl.ds(at, step), :]
    columns = held_ref[0, :, pl.ds(at, step)]
    left = lax.dot_general(part, held, (((1,), (1,)), ((), ())), preferred_element_type=F32)
    nl_ref[0] = DECAY * lstat_ref[0] + (1.0 - DECAY) * left
    right = lax.dot_general(columns, held, (((0,), (0,)), ((), ())), preferred_element_type=F32)
    nr_ref[0] = DECAY * rstat_ref[0] + (1.0 - DECAY) * right
    wide = part.astype(F32)
    moment = DECAY * moment_ref[0] + (1.0 - DECAY) * (wide * wide)
    nm_ref[0] = moment
    adam = wide / (jnp.sqrt(moment) + TINY)
    first = jnp.dot(lroot_ref[0], held, preferred_element_type=F32)
    high = first.astype(BF)
    low = (first - high.astype(F32)).astype(BF)
    direction = jnp.dot(high, rroot_ref[0], preferred_element_type=F32)
    direction += jnp.dot(low, rroot_ref[0], preferred_element_type=F32)
    dir_ref[0] = direction.astype(BF)
    width = wide.shape[1]

    @pl.when(r == 0)
    def _():
        acc[...] = jnp.zeros_like(acc)

    acc[0] += jnp.sum((adam * adam).reshape(step // 8, 8, width), axis=0)
    acc[1] += jnp.sum((direction * direction).reshape(step // 8, 8, width), axis=0)

    @pl.when((s == 0) & (r == 0))
    def _():
        norm_ref[...] = jnp.zeros_like(norm_ref)

    @pl.when(r == pl.num_programs(1) - 1)
    def _():
        row = lax.broadcasted_iota(jnp.int32, norm_ref.shape, 0)
        lane = lax.broadcasted_iota(jnp.int32, norm_ref.shape, 1)
        here = lane == param_ref[s]
        total = jnp.where(row == 0, jnp.sum(acc[0]), jnp.sum(acc[1]))
        norm_ref[...] += jnp.where(here & (row < 2), total, 0.0)


def slot_step(slot_param, held, lroot, rroot, lstat, rstat, moment):
    slots, block, width = held.shape
    step = min(128, block)
    whole = pl.BlockSpec((1, block, width), lambda s, r: (s, 0, 0))
    strip = pl.BlockSpec((1, step, width), lambda s, r: (s, r, 0))
    big = jax.ShapeDtypeStruct((slots, block, width), F32)
    return pl.pallas_call(
        slot_kernel,
        grid=(slots, block // step),
        out_shape=(
            big, big, big,
            jax.ShapeDtypeStruct((slots, block, width), BF),
            jax.ShapeDtypeStruct((8, 128), F32),
        ),
        in_specs=[
            pl.BlockSpec(memory_space=pltpu.SMEM), whole, strip, whole, strip, strip, strip,
        ],
        out_specs=(strip, strip, strip, strip, pl.BlockSpec((8, 128), lambda s, r: (0, 0))),
        scratch_shapes=[pltpu.VMEM((2, 8, width), F32)],
        compiler_params=pltpu.CompilerParams(dimension_semantics=("arbitrary", "arbitrary")),
        name="slot_step",
    )(slot_param, held, lroot, rroot, lstat, rstat, moment)


def gather_kernel(
    nblk, na_blk, n_shard, place_ref, norm_ref, dir_ref, out_ref, total_ref,
    slots, norms, group, columns, send_sem, recv_sem,
):
    y, x, c = position()
    mine = flat(y, x, c)
    shard = lax.axis_index("shard")
    nb_blk = nblk - na_blk
    rows = slots.shape[2]
    half = rows // 2
    ox, oc = 1 - x, 1 - c
    up, down, across = (y + 1) % NY, (y + 3) % NY, (y + 2) % NY
    A = pl.ds(0, na_blk)
    B = pl.ds(na_blk, nb_blk)
    ALL = pl.ds(0, nblk)
    H = (pl.ds(0, half), pl.ds(half, half))

    barrier = pltpu.get_barrier_semaphore()
    for dy, dx, dc in OFFSETS:
        pl.semaphore_signal(
            barrier, inc=1, device_id={"dp": flat(y + dy, x + dx, c + dc)},
            device_id_type=pl.DeviceIdType.MESH,
        )
    for k in range(1, n_shard):
        pl.semaphore_signal(
            barrier, inc=1, device_id={"shard": (shard + k) % n_shard},
            device_id_type=pl.DeviceIdType.MESH,
        )
    pl.semaphore_wait(barrier, len(OFFSETS) + n_shard - 1)

    copies = Copies(send_sem, recv_sem)
    first, second = [], []
    for dy, dx, dc in OFFSETS:
        q = flat(y + dy, x + dx, c + dc)
        first.append(copies.start(norm_ref, norms.at[mine], {"dp": q}))
    for dy, dx, dc in OFFSETS:
        qy, qx, qc = (y + dy) % NY, (x + dx) % NX, (c + dc) % NC
        second.append(
            copies.start(dir_ref.at[:, qc, qy, qx], slots.at[mine], {"dp": flat(qy, qx, qc)})
        )
    norms[mine] = norm_ref[...]
    slots[mine] = dir_ref[:, c, y, x]
    for copy in first:
        copy.wait_recv()
    total = norms[0]
    for i in range(1, norms.shape[0]):
        total = total + norms[i]
    group[...] = total
    third = [
        copies.start(group, columns.at[shard], {"shard": (shard + k) % n_shard})
        for k in range(1, n_shard)
    ]
    columns[shard] = total

    for copy in second:
        copy.wait_recv()
    for b in range(nblk):
        place = place_ref[b]
        out_ref[b, c, y, x] = slots[place // 2, place % 2]

    to_core = {"dp": flat(y, x, oc)}
    to_x = {"dp": flat(y, ox, c)}
    to_up = {"dp": flat(up, x, c)}
    to_down = {"dp": flat(down, x, c)}
    arrivals = []

    def pass_on(where, *index):
        part = out_ref.at[index]
        return copies.start(part, part, where)

    def across_cores(*index):
        arrivals.append(pass_on(to_core, *index))

    xa = pass_on(to_x, A, c, y, x)
    b_near = [pass_on(to_up, B, c, y, x), pass_on(to_down, B, c, y, x)]
    xb = [pass_on(to_x, B, c, y, x)]
    a_near = [pass_on(to_up, A, c, y, x), pass_on(to_down, A, c, y, x)]
    across_cores(ALL, c, y, x)

    b_near[0].wait_recv()
    b_far = [pass_on(to_up, B, c, down, x, H[0])]
    xb.append(pass_on(to_x, B, c, down, x))
    b_near[1].wait_recv()
    b_far.append(pass_on(to_down, B, c, up, x, H[1]))
    xb.append(pass_on(to_x, B, c, up, x))
    across_cores(B, c, down, x)
    across_cores(B, c, up, x)

    xa.wait_recv()
    a_next = [pass_on(to_up, A, c, y, ox), pass_on(to_down, A, c, y, ox)]
    across_cores(A, c, y, ox)

    a_near[0].wait_recv()
    a_far = [pass_on(to_up, A, c, down, x)]
    across_cores(A, c, down, x)
    a_near[1].wait_recv()
    across_cores(A, c, up, x)

    b_far[0].wait_recv()
    b_far[1].wait_recv()
    xb.append(pass_on(to_x, B, c, across, x))
    across_cores(B, c, across, x)

    a_next[1].wait_recv()
    a_far.append(pass_on(to_down, A, c, up, ox))
    across_cores(A, c, up, ox)
    a_next[0].wait_recv()
    across_cores(A, c, down, ox)

    for copy in third:
        copy.wait_recv()
    total = columns[0]
    for i in range(1, n_shard):
        total = total + columns[i]
    total_ref[...] = total

    for i, chunk in enumerate((y, down, up)):
        xb[i].wait_recv()
        across_cores(B, c, chunk, ox)
    a_far[0].wait_recv()
    across_cores(A, c, across, x)
    a_far[1].wait_recv()
    across_cores(A, c, across, ox)
    xb[3].wait_recv()
    across_cores(B, c, across, ox)
    for copy in arrivals:
        copy.wait_recv()
    copies.finish()


def gather_blocks(direction, places, norm, n_shard):
    slots, block, width = direction.shape
    nblk = places.shape[0]
    rows = block // (NY * NX * NC)
    na_blk = (nblk + 1) // 2
    n_dev = NY * NX * NC
    n_copies = 2 * len(OFFSETS) + n_shard - 1 + 1 + 2 + 4 + 2 + 2 + 2 + 2 + 15
    out, total = pl.pallas_call(
        functools.partial(gather_kernel, nblk, na_blk, n_shard),
        out_shape=(
            jax.ShapeDtypeStruct((nblk, NC, NY, NX, rows, width), BF),
            jax.ShapeDtypeStruct(norm.shape, F32),
        ),
        in_specs=[
            pl.BlockSpec(memory_space=pltpu.SMEM),
            pl.BlockSpec(memory_space=pltpu.VMEM),
            pl.BlockSpec(memory_space=pltpu.VMEM),
        ],
        out_specs=(
            pl.BlockSpec(memory_space=pltpu.VMEM),
            pl.BlockSpec(memory_space=pltpu.VMEM),
        ),
        scratch_shapes=[
            pltpu.VMEM((n_dev, slots, rows, width), BF),
            pltpu.VMEM((n_dev,) + norm.shape, F32),
            pltpu.VMEM(norm.shape, F32),
            pltpu.VMEM((n_shard,) + norm.shape, F32),
            pltpu.SemaphoreType.DMA((n_copies,)),
            pltpu.SemaphoreType.DMA((n_copies,)),
        ],
        compiler_params=pltpu.CompilerParams(collective_id=1, has_side_effects=True),
        name="gather_blocks",
    )(places, norm, direction.reshape(slots, NC, NY, NX, rows, width))
    return out.reshape(nblk, block, width), total


def on_device(gradients, owners, block_param, left_stat, right_stat, moment, left_root, right_root):
    replicas = lax.axis_size("dp")
    n_shard = lax.axis_size("shard")
    capacity = left_stat.shape[0]
    blocks = gradients.shape[1]
    device = lax.axis_index("dp")
    column = lax.axis_index("shard")
    owner_row = owners[0]
    counter = jnp.arange(blocks, dtype=jnp.int32)
    same_owner = owner_row[:, None] == owner_row[None, :]
    earlier = counter[None, :] < counter[:, None]
    places = owner_row * capacity + jnp.sum(
        jnp.where(same_owner & earlier, 1, 0), axis=1
    ).astype(jnp.int32)
    slot_ids = jnp.arange(replicas * capacity, dtype=jnp.int32)
    matches = places[None, :] == slot_ids[:, None]
    source = jnp.min(jnp.where(matches, counter[None, :], blocks), axis=1)
    local_params = lax.dynamic_slice_in_dim(block_param, column * blocks, blocks, 0)
    my_ids = device * capacity + jnp.arange(capacity, dtype=jnp.int32)
    mine = places[None, :] == my_ids[:, None]
    slot_param = jnp.max(jnp.where(mine, local_params[None, :], -1), axis=1)

    held = reduce_to_owners(gradients[0], source)
    new_left, new_right, new_moment, direction, norm = slot_step(
        slot_param, held, left_root[:, 0], right_root[:, 0],
        left_stat[:, 0], right_stat[:, 0], moment[:, 0],
    )
    gathered, total = gather_blocks(direction, places, norm, n_shard)
    graft_ratio = jnp.sqrt((total[0, :NPARAM] + TINY) / (total[1, :NPARAM] + TINY))
    param_ids = jnp.arange(NPARAM, dtype=jnp.int32)
    member = local_params[:, None] == param_ids[None, :]
    block_ratio = jnp.sum(jnp.where(member, graft_ratio[None, :], 0.0), axis=1)
    update = (block_ratio[:, None, None] * gathered.astype(F32)).astype(BF)
    return (new_left[:, None], new_right[:, None], new_moment[:, None], update)


def solution(mesh):
    state = P("dp", "shard", None, None)
    return jax.shard_map(
        on_device,
        mesh=mesh,
        in_specs=(state, P("shard", None), P(), state, state, state, state, state),
        out_specs=(state, state, state, P("shard", None, None)),
        check_vma=False,
    )
```

```python
import functools

import jax
import jax.numpy as jnp
from jax import lax
from jax.experimental import pallas as pl
from jax.experimental.pallas import tpu as pltpu
from jax.sharding import PartitionSpec as P

DECAY = 0.95
TINY = 1e-06
NY, NX, NC = 4, 2, 2
GRANT = 30 << 20
BF = jnp.bfloat16
F32 = jnp.float32


def position():
    d = lax.axis_index("dp")
    return d // 4, (d // 2) % 2, d % 2


def flat(y, x, c):
    return (y % NY) * 4 + (x % NX) * 2 + c % NC


OFFSETS = [
    (dy, dx, dc)
    for dy in (2, 1, 3, 0)
    for dx in (1, 0)
    for dc in (0, 1)
    if (dy, dx, dc) != (0, 0, 0)
]


def slot_places(owner_ref, nblk):
    owners = [owner_ref[0, b] for b in range(nblk)]
    places = []
    for b in range(nblk):
        place = owners[b] * 2
        for other in range(b):
            place = place + jnp.where(owners[other] == owners[b], 1, 0)
        places.append(place)
    return places


class Copies:
    def __init__(self, send, recv):
        self.send, self.recv, self.count, self.all = send, recv, 0, []

    def start(self, src, dst, where):
        i = self.count
        self.count += 1
        copy = pltpu.make_async_remote_copy(
            src_ref=src,
            dst_ref=dst,
            send_sem=self.send.at[i],
            recv_sem=self.recv.at[i],
            device_id=where,
            device_id_type=pl.DeviceIdType.MESH,
        )
        copy.start()
        self.all.append(copy)
        return copy

    def finish(self):
        for copy in self.all:
            copy.wait_send()


def add_blocks(count, out, first, second):
    def body(b, carry):
        out[b] = first[b] + second[b]
        return carry

    lax.fori_loop(0, count, body, 0)


def add_many(count, out, *terms):
    def body(b, carry):
        total = terms[0][b].astype(F32)
        for term in terms[1:]:
            total = total + term[b].astype(F32)
        out[b] = total.astype(BF)
        return carry

    lax.fori_loop(0, count, body, 0)


def step_kernel(
    nblk, na_blk, n_shard, owner_hbm, param_hbm, grad_ref, lstat_hbm, rstat_hbm, moment_hbm,
    lroot_hbm, rroot_hbm, nl_ref, nr_ref, nm_ref, out_ref,
    loc, grad, rem, far_a, mid_b, near_a, mid_a, far_b, near_b, share, stage,
    held, lroot, rroot, direct, acc, norm_ref, slots, norms, group, columns,
    source_ref, owner_ref, param_ref, local_sem, state_sem, send_sem, recv_sem,
):
    y, x, c = position()
    mine = flat(y, x, c)
    shard = lax.axis_index("shard")
    nb_blk = nblk - na_blk
    rows = share.shape[1]
    half = rows // 2
    ox, oc = 1 - x, 1 - c
    up, down, across = (y + 1) % NY, (y + 3) % NY, (y + 2) % NY
    A = pl.ds(0, na_blk)
    B = pl.ds(na_blk, nb_blk)
    ALL = pl.ds(0, nblk)
    H = (pl.ds(0, half), pl.ds(half, half))

    def gpart(which, core, buf=grad):
        return [
            buf.at[A, core, across],
            buf.at[B, core, :, ox],
            buf.at[A, core, up],
            buf.at[A, core, down],
            buf.at[B, core, :, x],
            buf.at[A, core, y],
        ][which]

    def vpart(buf, which):
        return [
            buf.at[A, across],
            buf.at[B, :, ox],
            buf.at[A, up],
            buf.at[A, down],
            buf.at[B, :, x],
            buf.at[A, y],
        ][which]

    loads = {}
    for i in range(6):
        for own, core in enumerate((oc, c)):
            load = pltpu.make_async_copy(
                gpart(i, core, grad_ref), gpart(i, core), local_sem.at[i, own]
            )
            load.start()
            loads[i, own] = load
    states = [
        pltpu.make_async_copy(src, dst, state_sem.at[i])
        for i, (src, dst) in enumerate((
            (lroot_hbm, lroot), (rroot_hbm, rroot), (moment_hbm, nm_ref),
            (lstat_hbm, nl_ref), (rstat_hbm, nr_ref),
            (owner_hbm, owner_ref), (param_hbm, param_ref),
        ))
    ]
    for load in states:
        load.start()

    barrier = pltpu.get_barrier_semaphore()
    for dy, dx, dc in OFFSETS:
        pl.semaphore_signal(
            barrier, inc=1, device_id={"dp": flat(y + dy, x + dx, c + dc)},
            device_id_type=pl.DeviceIdType.MESH,
        )
    for k in range(1, n_shard):
        pl.semaphore_signal(
            barrier, inc=1, device_id={"shard": (shard + k) % n_shard},
            device_id_type=pl.DeviceIdType.MESH,
        )
    pl.semaphore_wait(barrier, len(OFFSETS) + n_shard - 1)

    to_core = {"dp": flat(y, x, oc)}
    to_x = {"dp": flat(y, ox, c)}
    to_up = {"dp": flat(up, x, c)}
    to_down = {"dp": flat(down, x, c)}
    copies = Copies(send_sem, recv_sem)
    pair = []
    for i in range(6):
        loads[i, 0].wait()
        pair.append(copies.start(gpart(i, oc), vpart(rem, i), to_core))

    def pair_sum(i):
        loads[i, 1].wait()
        pair[i].wait_recv()
        out, mine, other = vpart(loc, i), gpart(i, c), vpart(rem, i)
        inner = mine.shape[1]
        for j in range(inner):
            add_blocks(out.shape[0], out.at[:, j], mine.at[:, j], other.at[:, j])

    pair_sum(0)
    fa = [
        copies.start(loc.at[A, across, 0], far_a.at[0], to_up),
        copies.start(loc.at[A, across, 1], far_a.at[1], to_down),
    ]
    pair_sum(1)
    mb = [
        copies.start(loc.at[B, chunk, ox], mid_b.at[:, chunk], to_x)
        for chunk in (across, up, down, y)
    ]
    pair_sum(2)
    n_a = {(0, 1): copies.start(loc.at[A, up, 1], near_a.at[0, 1], to_up)}
    pair_sum(3)
    n_a[1, 0] = copies.start(loc.at[A, down, 0], near_a.at[1, 0], to_down)
    pair_sum(4)
    pair_sum(5)

    for load in states[5:]:
        load.wait()
    places = slot_places(owner_ref, nblk)

    def find(slot, carry):
        block = nblk
        for b in range(nblk):
            block = jnp.where(places[b] == slot, b, block)
        source_ref[slot] = block
        return carry

    lax.fori_loop(0, 2 * NY * NX * NC, find, 0)

    fa[0].wait_recv()
    add_blocks(na_blk, loc.at[A, up, 0], loc.at[A, up, 0], far_a.at[0])
    n_a[0, 0] = copies.start(loc.at[A, up, 0], near_a.at[0, 0], to_up)
    fa[1].wait_recv()
    add_blocks(na_blk, loc.at[A, down, 1], loc.at[A, down, 1], far_a.at[1])
    n_a[1, 1] = copies.start(loc.at[A, down, 1], near_a.at[1, 1], to_down)

    def middle(i, chunk):
        mb[i].wait_recv()
        add_blocks(nb_blk, loc.at[B, chunk, x], loc.at[B, chunk, x], mid_b.at[:, chunk])

    middle(0, across)
    fb = [
        copies.start(loc.at[B, across, x, H[0]], far_b.at[0], to_up),
        copies.start(loc.at[B, across, x, H[1]], far_b.at[1], to_down),
    ]
    middle(1, up)
    n_b = {(0, 1): copies.start(loc.at[B, up, x, H[1]], near_b.at[0, 1], to_up)}
    middle(2, down)
    n_b[1, 0] = copies.start(loc.at[B, down, x, H[0]], near_b.at[1, 0], to_down)

    for key in ((0, 1), (1, 0), (0, 0), (1, 1)):
        n_a[key].wait_recv()
    add_many(na_blk, loc.at[A, y, ox], loc.at[A, y, ox], near_a.at[0, ox], near_a.at[1, ox])
    ma = copies.start(loc.at[A, y, ox], mid_a, to_x)

    fb[0].wait_recv()
    add_blocks(nb_blk, loc.at[B, up, x, H[0]], loc.at[B, up, x, H[0]], far_b.at[0])
    n_b[0, 0] = copies.start(loc.at[B, up, x, H[0]], near_b.at[0, 0], to_up)
    fb[1].wait_recv()
    add_blocks(nb_blk, loc.at[B, down, x, H[1]], loc.at[B, down, x, H[1]], far_b.at[1])
    n_b[1, 1] = copies.start(loc.at[B, down, x, H[1]], near_b.at[1, 1], to_down)

    share[nblk] = jnp.zeros(share.shape[1:], BF)
    ma.wait_recv()
    add_many(
        na_blk, share.at[A], loc.at[A, y, x], near_a.at[0, x], near_a.at[1, x], mid_a
    )
    mb[3].wait_recv()
    for key in ((0, 1), (1, 0), (0, 0), (1, 1)):
        n_b[key].wait_recv()
    for h in range(2):
        add_many(
            nb_blk, share.at[B, H[h]], loc.at[B, y, x, H[h]], mid_b.at[:, y, H[h]],
            near_b.at[0, h], near_b.at[1, h],
        )

    sent = []
    for k, (dy, dx, dc) in enumerate(OFFSETS):
        q = flat(y + dy, x + dx, c + dc)
        for j in range(2):
            stage[k, j] = share[source_ref[q * 2 + j]]
        sent.append(copies.start(stage.at[k], held.at[:, c, y, x], {"dp": q}))
    for j in range(2):
        held[j, c, y, x] = share[source_ref[mine * 2 + j]]
    for load in states[:3]:
        load.wait()
    for copy in sent:
        copy.wait_recv()

    step = 2 * NX * rows
    width = held.shape[-1]
    block = 4 * step

    def whole(j):
        return held[j].reshape(block, width)

    def strip_of(j, r):
        return held[j, r // 2, pl.ds(2 * (r % 2), 2)].reshape(step, width)

    acc[...] = jnp.zeros_like(acc)

    def precondition(i, carry):
        j, r = i // 4, i % 4
        at = pl.ds(pl.multiple_of(r * step, step), step)
        left = jnp.dot(lroot[j, at], whole(j), preferred_element_type=F32)
        high = left.astype(BF)
        low = (left - high.astype(F32)).astype(BF)
        direction = jnp.dot(high, rroot[j], preferred_element_type=F32)
        direction += jnp.dot(low, rroot[j], preferred_element_type=F32)
        part = direction.astype(BF).reshape(2, NX, rows, width)
        direct[j, r // 2, pl.ds(2 * (r % 2), 2)] = part
        wide = strip_of(j, r).astype(F32)
        moment = DECAY * nm_ref[j, at] + (1.0 - DECAY) * (wide * wide)
        nm_ref[j, at] = moment
        adam = wide / (jnp.sqrt(moment) + TINY)
        acc[j, 0] += jnp.sum((adam * adam).reshape(step // 8, 8, width), axis=0)
        acc[j, 1] += jnp.sum((direction * direction).reshape(step // 8, 8, width), axis=0)
        return carry

    lax.fori_loop(0, 8, precondition, 0)

    tile = (8, 128)
    row = lax.broadcasted_iota(jnp.int32, tile, 0)
    lane = lax.broadcasted_iota(jnp.int32, tile, 1)
    local = jnp.zeros(tile, F32)
    for j in range(2):
        block_at = source_ref[mine * 2 + j]
        param = param_ref[shard * nblk + jnp.minimum(block_at, nblk - 1)]
        param = jnp.where(block_at < nblk, param, -1)
        sums = jnp.where(row == 0, jnp.sum(acc[j, 0]), jnp.sum(acc[j, 1]))
        local = local + jnp.where((lane == param) & (row < 2), sums, 0.0)
    norm_ref[...] = local

    first, second = [], []
    for dy, dx, dc in OFFSETS:
        q = flat(y + dy, x + dx, c + dc)
        first.append(copies.start(norm_ref, norms.at[mine], {"dp": q}))
    for dy, dx, dc in OFFSETS:
        qy, qx, qc = (y + dy) % NY, (x + dx) % NX, (c + dc) % NC
        second.append(
            copies.start(direct.at[:, qc, qy, qx], slots.at[mine], {"dp": flat(qy, qx, qc)})
        )
    norms[mine] = norm_ref[...]
    slots[mine] = direct[:, c, y, x]
    for load in states[3:5]:
        load.wait()

    def gram(i, carry):
        j, r = i // 4, i % 4
        at = pl.ds(pl.multiple_of(r * step, step), step)
        left = lax.dot_general(
            strip_of(j, r), whole(j), (((1,), (1,)), ((), ())), preferred_element_type=F32
        )
        nl_ref[j, at] = DECAY * nl_ref[j, at] + (1.0 - DECAY) * left
        columns_of = held[j, :, :, :, :, at].reshape(block, step)
        right = lax.dot_general(
            columns_of, whole(j), (((0,), (0,)), ((), ())), preferred_element_type=F32
        )
        nr_ref[j, at] = DECAY * nr_ref[j, at] + (1.0 - DECAY) * right
        return carry

    lax.fori_loop(0, 2, gram, 0)
    for copy in first:
        copy.wait_recv()
    total = norms[0]
    for i in range(1, norms.shape[0]):
        total = total + norms[i]
    group[...] = total
    third = [
        copies.start(group, columns.at[shard], {"shard": (shard + k) % n_shard})
        for k in range(1, n_shard)
    ]
    columns[shard] = total

    lax.fori_loop(2, 8, gram, 0)

    for copy in third:
        copy.wait_recv()
    total = columns[0]
    for i in range(1, n_shard):
        total = total + columns[i]
    ratio = jnp.sqrt((total[0:1] + TINY) / (total[1:2] + TINY))
    for copy in second:
        copy.wait_recv()
    for b in range(nblk):
        place = places[b]
        param = param_ref[shard * nblk + b]
        scale = jnp.sum(jnp.where(lane[0:1] == param, ratio, 0.0), axis=1, keepdims=True)
        out_ref[b, c, y, x] = (scale * slots[place // 2, place % 2].astype(F32)).astype(BF)

    arrivals = []

    def pass_on(where, *index):
        part = out_ref.at[index]
        return copies.start(part, part, where)

    def across_cores(*index):
        arrivals.append(pass_on(to_core, *index))

    xa = pass_on(to_x, A, c, y, x)
    b_near = [pass_on(to_up, B, c, y, x), pass_on(to_down, B, c, y, x)]
    xb = [pass_on(to_x, B, c, y, x)]
    a_near = [pass_on(to_up, A, c, y, x), pass_on(to_down, A, c, y, x)]
    across_cores(ALL, c, y, x)

    b_near[0].wait_recv()
    b_far = [pass_on(to_up, B, c, down, x, H[0])]
    xb.append(pass_on(to_x, B, c, down, x))
    b_near[1].wait_recv()
    b_far.append(pass_on(to_down, B, c, up, x, H[1]))
    xb.append(pass_on(to_x, B, c, up, x))
    across_cores(B, c, down, x)
    across_cores(B, c, up, x)

    xa.wait_recv()
    a_next = [pass_on(to_up, A, c, y, ox), pass_on(to_down, A, c, y, ox)]
    across_cores(A, c, y, ox)

    a_near[0].wait_recv()
    a_far = [pass_on(to_up, A, c, down, x)]
    across_cores(A, c, down, x)
    a_near[1].wait_recv()
    across_cores(A, c, up, x)

    b_far[0].wait_recv()
    b_far[1].wait_recv()
    xb.append(pass_on(to_x, B, c, across, x))
    across_cores(B, c, across, x)

    a_next[1].wait_recv()
    a_far.append(pass_on(to_down, A, c, up, ox))
    across_cores(A, c, up, ox)
    a_next[0].wait_recv()
    across_cores(A, c, down, ox)

    for i, chunk in enumerate((y, down, up)):
        xb[i].wait_recv()
        across_cores(B, c, chunk, ox)
    a_far[0].wait_recv()
    across_cores(A, c, across, x)
    a_far[1].wait_recv()
    across_cores(A, c, across, ox)
    xb[3].wait_recv()
    across_cores(B, c, across, ox)
    for copy in arrivals:
        copy.wait_recv()
    copies.finish()


def flush_kernel(*refs):
    count = len(refs) // 2
    sem = refs[-1]
    copies = [
        pltpu.make_async_copy(refs[i], refs[count + i], sem.at[i]) for i in range(count)
    ]
    for copy in copies:
        copy.start()
    for copy in copies:
        copy.wait()


def flush(*arrays):
    return pl.pallas_call(
        flush_kernel,
        out_shape=tuple(jax.ShapeDtypeStruct(a.shape, a.dtype) for a in arrays),
        in_specs=[pl.BlockSpec(memory_space=pltpu.VMEM)] * len(arrays),
        out_specs=tuple(pl.BlockSpec(memory_space=pltpu.HBM) for _ in arrays),
        scratch_shapes=[pltpu.SemaphoreType.DMA((len(arrays),))],
        compiler_params=pltpu.CompilerParams(vmem_limit_bytes=GRANT),
        name="flush",
    )(*arrays)


def on_device(gradients, owners, block_param, left_stat, right_stat, moment, left_root, right_root):
    _, nblk, block, width = gradients.shape
    n_shard = lax.axis_size("shard")
    n_dev = NY * NX * NC
    rows = block // n_dev
    na_blk = (nblk + 1) // 2
    nb_blk = nblk - na_blk
    n_copies = 23 + 3 * len(OFFSETS) + n_shard - 1 + 15 + 15
    state = jax.ShapeDtypeStruct((2, block, width), F32)
    hbm = pl.BlockSpec(memory_space=pltpu.HBM)
    vmem = pl.BlockSpec(memory_space=pltpu.VMEM)
    slot_rows = (2, NC, NY, NX, rows, width)
    new_left, new_right, new_moment, update = pl.pallas_call(
        functools.partial(step_kernel, nblk, na_blk, n_shard),
        out_shape=(
            state, state, state,
            jax.ShapeDtypeStruct((nblk, NC, NY, NX, rows, width), BF),
        ),
        in_specs=[hbm] * 8,
        out_specs=(vmem, vmem, vmem, vmem),
        scratch_shapes=[
            pltpu.VMEM((nblk, NY, NX, rows, width), BF),
            pltpu.VMEM((nblk, NC, NY, NX, rows, width), BF),
            pltpu.VMEM((nblk, NY, NX, rows, width), BF),
            pltpu.VMEM((2, na_blk, rows, width), BF),
            pltpu.VMEM((nb_blk, NY, rows, width), BF),
            pltpu.VMEM((2, 2, na_blk, rows, width), BF),
            pltpu.VMEM((na_blk, rows, width), BF),
            pltpu.VMEM((2, nb_blk, rows // 2, width), BF),
            pltpu.VMEM((2, 2, nb_blk, rows // 2, width), BF),
            pltpu.VMEM((nblk + 1, rows, width), BF),
            pltpu.VMEM((len(OFFSETS), 2, rows, width), BF),
            pltpu.VMEM(slot_rows, BF),
            pltpu.VMEM((2, block, width), BF),
            pltpu.VMEM((2, block, width), BF),
            pltpu.VMEM(slot_rows, BF),
            pltpu.VMEM((2, 2, 8, width), F32),
            pltpu.VMEM((8, 128), F32),
            pltpu.VMEM((n_dev, 2, rows, width), BF),
            pltpu.VMEM((n_dev, 8, 128), F32),
            pltpu.VMEM((8, 128), F32),
            pltpu.VMEM((n_shard, 8, 128), F32),
            pltpu.SMEM((2 * n_dev,), jnp.int32),
            pltpu.SMEM(owners.shape, jnp.int32),
            pltpu.SMEM(block_param.shape, jnp.int32),
            pltpu.SemaphoreType.DMA((6, 2)),
            pltpu.SemaphoreType.DMA((7,)),
            pltpu.SemaphoreType.DMA((n_copies,)),
            pltpu.SemaphoreType.DMA((n_copies,)),
        ],
        compiler_params=pltpu.CompilerParams(
            collective_id=0, has_side_effects=True, vmem_limit_bytes=GRANT
        ),
        name="shampoo_step",
    )(
        *(
            pltpu.with_memory_space_constraint(array, pltpu.HBM)
            for array in (
                owners, block_param,
                gradients.reshape(nblk, NC, NY, NX, rows, width),
                left_stat[:, 0], right_stat[:, 0], moment[:, 0], left_root[:, 0], right_root[:, 0],
            )
        ),
    )
    new_left, new_right, new_moment, update = flush(new_left, new_right, new_moment, update)
    return (
        new_left[:, None], new_right[:, None], new_moment[:, None],
        update.reshape(nblk, block, width),
    )


def solution(mesh):
    state = P("dp", "shard", None, None)
    return jax.shard_map(
        on_device,
        mesh=mesh,
        in_specs=(state, P("shard", None), P(), state, state, state, state, state),
        out_specs=(state, state, state, P("shard", None, None)),
        check_vma=False,
    )
```

```python
import functools

import jax
import jax.numpy as jnp
from jax import lax
from jax.experimental import pallas as pl
from jax.experimental.pallas import tpu as pltpu
from jax.sharding import PartitionSpec as P

DECAY = 0.95
TINY = 1e-06
NY, NX, NC = 4, 2, 2
GRANT = 30 << 20
BF = jnp.bfloat16
F32 = jnp.float32


def position():
    d = lax.axis_index("dp")
    return d // 4, (d // 2) % 2, d % 2


def flat(y, x, c):
    return (y % NY) * 4 + (x % NX) * 2 + c % NC


OFFSETS = [
    (dy, dx, dc)
    for dy in (2, 1, 3, 0)
    for dx in (1, 0)
    for dc in (0, 1)
    if (dy, dx, dc) != (0, 0, 0)
]


def slot_places(owner_ref, nblk):
    owners = [owner_ref[0, b] for b in range(nblk)]
    places = []
    for b in range(nblk):
        place = owners[b] * 2
        for other in range(b):
            place = place + jnp.where(owners[other] == owners[b], 1, 0)
        places.append(place)
    return places


class Copies:
    def __init__(self, send, recv):
        self.send, self.recv, self.count, self.all = send, recv, 0, []

    def start(self, src, dst, where):
        i = self.count
        self.count += 1
        copy = pltpu.make_async_remote_copy(
            src_ref=src,
            dst_ref=dst,
            send_sem=self.send.at[i],
            recv_sem=self.recv.at[i],
            device_id=where,
            device_id_type=pl.DeviceIdType.MESH,
        )
        copy.start()
        self.all.append(copy)
        return copy

    def finish(self):
        for copy in self.all:
            copy.wait_send()


def add_blocks(count, out, first, second):
    def body(b, carry):
        out[b] = first[b] + second[b]
        return carry

    lax.fori_loop(0, count, body, 0)


def add_many(count, out, *terms):
    def body(b, carry):
        total = terms[0][b].astype(F32)
        for term in terms[1:]:
            total = total + term[b].astype(F32)
        out[b] = total.astype(BF)
        return carry

    lax.fori_loop(0, count, body, 0)


def step_kernel(
    nblk, na_blk, n_shard, owner_hbm, param_hbm, grad_ref, lstat_hbm, rstat_hbm, moment_hbm,
    lroot_hbm, rroot_hbm, nl_ref, nr_ref, nm_ref, out_ref,
    loc, grad, rem, far_a, mid_b, near_a, mid_a, far_b, near_b, share, stage,
    held, lroot, rroot, direct, acc, norm_ref, slots, norms, group, columns,
    source_ref, owner_ref, param_ref, local_sem, state_sem, send_sem, recv_sem,
):
    y, x, c = position()
    mine = flat(y, x, c)
    shard = lax.axis_index("shard")
    nb_blk = nblk - na_blk
    rows = share.shape[1]
    half = rows // 2
    ox, oc = 1 - x, 1 - c
    up, down, across = (y + 1) % NY, (y + 3) % NY, (y + 2) % NY
    A = pl.ds(0, na_blk)
    B = pl.ds(na_blk, nb_blk)
    ALL = pl.ds(0, nblk)
    H = (pl.ds(0, half), pl.ds(half, half))

    def gpart(which, core, buf=grad):
        return [
            buf.at[A, core, across],
            buf.at[B, core, :, ox],
            buf.at[A, core, up],
            buf.at[A, core, down],
            buf.at[B, core, :, x],
            buf.at[A, core, y],
        ][which]

    def vpart(buf, which):
        return [
            buf.at[A, across],
            buf.at[B, :, ox],
            buf.at[A, up],
            buf.at[A, down],
            buf.at[B, :, x],
            buf.at[A, y],
        ][which]

    loads = {}
    for i in range(6):
        for own, core in enumerate((oc, c)):
            load = pltpu.make_async_copy(
                gpart(i, core, grad_ref), gpart(i, core), local_sem.at[i, own]
            )
            load.start()
            loads[i, own] = load
    states = [
        pltpu.make_async_copy(src, dst, state_sem.at[i])
        for i, (src, dst) in enumerate((
            (lroot_hbm, lroot), (rroot_hbm, rroot), (moment_hbm, nm_ref),
            (lstat_hbm, nl_ref), (rstat_hbm, nr_ref),
            (owner_hbm, owner_ref), (param_hbm, param_ref),
        ))
    ]

    barrier = pltpu.get_barrier_semaphore()
    for dy, dx, dc in OFFSETS:
        pl.semaphore_signal(
            barrier, inc=1, device_id={"dp": flat(y + dy, x + dx, c + dc)},
            device_id_type=pl.DeviceIdType.MESH,
        )
    for k in range(1, n_shard):
        pl.semaphore_signal(
            barrier, inc=1, device_id={"shard": (shard + k) % n_shard},
            device_id_type=pl.DeviceIdType.MESH,
        )
    pl.semaphore_wait(barrier, len(OFFSETS) + n_shard - 1)

    to_core = {"dp": flat(y, x, oc)}
    to_x = {"dp": flat(y, ox, c)}
    to_up = {"dp": flat(up, x, c)}
    to_down = {"dp": flat(down, x, c)}
    copies = Copies(send_sem, recv_sem)
    pair = []
    for i in range(6):
        loads[i, 0].wait()
        pair.append(copies.start(gpart(i, oc), vpart(rem, i), to_core))

    def pair_sum(i):
        loads[i, 1].wait()
        pair[i].wait_recv()
        out, mine, other = vpart(loc, i), gpart(i, c), vpart(rem, i)
        inner = mine.shape[1]
        for j in range(inner):
            add_blocks(out.shape[0], out.at[:, j], mine.at[:, j], other.at[:, j])

    for load in states:
        load.start()
    pair_sum(0)
    fa = [
        copies.start(loc.at[A, across, 0], far_a.at[0], to_up),
        copies.start(loc.at[A, across, 1], far_a.at[1], to_down),
    ]
    pair_sum(1)
    mb = [
        copies.start(loc.at[B, chunk, ox], mid_b.at[:, chunk], to_x)
        for chunk in (across, up, down, y)
    ]
    pair_sum(2)
    n_a = {(0, 1): copies.start(loc.at[A, up, 1], near_a.at[0, 1], to_up)}
    pair_sum(3)
    n_a[1, 0] = copies.start(loc.at[A, down, 0], near_a.at[1, 0], to_down)
    pair_sum(4)
    pair_sum(5)

    for load in states[5:]:
        load.wait()
    places = slot_places(owner_ref, nblk)

    def find(slot, carry):
        block = nblk
        for b in range(nblk):
            block = jnp.where(places[b] == slot, b, block)
        source_ref[slot] = block
        return carry

    lax.fori_loop(0, 2 * NY * NX * NC, find, 0)

    fa[0].wait_recv()
    add_blocks(na_blk, loc.at[A, up, 0], loc.at[A, up, 0], far_a.at[0])
    n_a[0, 0] = copies.start(loc.at[A, up, 0], near_a.at[0, 0], to_up)
    fa[1].wait_recv()
    add_blocks(na_blk, loc.at[A, down, 1], loc.at[A, down, 1], far_a.at[1])
    n_a[1, 1] = copies.start(loc.at[A, down, 1], near_a.at[1, 1], to_down)

    def middle(i, chunk):
        mb[i].wait_recv()
        add_blocks(nb_blk, loc.at[B, chunk, x], loc.at[B, chunk, x], mid_b.at[:, chunk])

    middle(0, across)
    fb = [
        copies.start(loc.at[B, across, x, H[0]], far_b.at[0], to_up),
        copies.start(loc.at[B, across, x, H[1]], far_b.at[1], to_down),
    ]
    middle(1, up)
    n_b = {(0, 1): copies.start(loc.at[B, up, x, H[1]], near_b.at[0, 1], to_up)}
    middle(2, down)
    n_b[1, 0] = copies.start(loc.at[B, down, x, H[0]], near_b.at[1, 0], to_down)

    for key in ((0, 1), (1, 0), (0, 0), (1, 1)):
        n_a[key].wait_recv()
    add_many(na_blk, loc.at[A, y, ox], loc.at[A, y, ox], near_a.at[0, ox], near_a.at[1, ox])
    ma = copies.start(loc.at[A, y, ox], mid_a, to_x)

    fb[0].wait_recv()
    add_blocks(nb_blk, loc.at[B, up, x, H[0]], loc.at[B, up, x, H[0]], far_b.at[0])
    n_b[0, 0] = copies.start(loc.at[B, up, x, H[0]], near_b.at[0, 0], to_up)
    fb[1].wait_recv()
    add_blocks(nb_blk, loc.at[B, down, x, H[1]], loc.at[B, down, x, H[1]], far_b.at[1])
    n_b[1, 1] = copies.start(loc.at[B, down, x, H[1]], near_b.at[1, 1], to_down)

    share[nblk] = jnp.zeros(share.shape[1:], BF)
    ma.wait_recv()
    add_many(
        na_blk, share.at[A], loc.at[A, y, x], near_a.at[0, x], near_a.at[1, x], mid_a
    )
    mb[3].wait_recv()
    for key in ((0, 1), (1, 0), (0, 0), (1, 1)):
        n_b[key].wait_recv()
    for h in range(2):
        add_many(
            nb_blk, share.at[B, H[h]], loc.at[B, y, x, H[h]], mid_b.at[:, y, H[h]],
            near_b.at[0, h], near_b.at[1, h],
        )

    sent = ([], [])
    for j in range(2):
        for k, (dy, dx, dc) in enumerate(OFFSETS):
            q = flat(y + dy, x + dx, c + dc)
            stage[k, j] = share[source_ref[q * 2 + j]]
            sent[j].append(copies.start(stage.at[k, j], held.at[j, c, y, x], {"dp": q}))
        held[j, c, y, x] = share[source_ref[mine * 2 + j]]
    for load in states[:3]:
        load.wait()
    step = 2 * NX * rows
    width = held.shape[-1]
    block = 4 * step

    def whole(j):
        return held[j].reshape(block, width)

    def strip_of(j, r):
        return held[j, r // 2, pl.ds(2 * (r % 2), 2)].reshape(step, width)

    acc[...] = jnp.zeros_like(acc)

    def precondition(j, r, carry):
        tall = 2 * step
        at = pl.ds(pl.multiple_of(r * tall, tall), tall)
        left = jnp.dot(lroot[j, at], whole(j), preferred_element_type=F32)
        high = left.astype(BF)
        low = (left - high.astype(F32)).astype(BF)
        direction = jnp.dot(high, rroot[j], preferred_element_type=F32)
        direction += jnp.dot(low, rroot[j], preferred_element_type=F32)
        direct[j, r] = direction.astype(BF).reshape(NY, NX, rows, width)
        wide = held[j, r].reshape(tall, width).astype(F32)
        moment = DECAY * nm_ref[j, at] + (1.0 - DECAY) * (wide * wide)
        nm_ref[j, at] = moment
        adam = wide / (jnp.sqrt(moment) + TINY)
        acc[j, 0] += jnp.sum((adam * adam).reshape(tall // 8, 8, width), axis=0)
        acc[j, 1] += jnp.sum((direction * direction).reshape(tall // 8, 8, width), axis=0)
        return carry

    second = []

    def send_out(j):
        for dy, dx, dc in OFFSETS:
            qy, qx, qc = (y + dy) % NY, (x + dx) % NX, (c + dc) % NC
            second.append(
                copies.start(
                    direct.at[j, qc, qy, qx], slots.at[mine, j], {"dp": flat(qy, qx, qc)}
                )
            )

    for copy in sent[0]:
        copy.wait_recv()
    lax.fori_loop(0, 2, functools.partial(precondition, 0), 0)
    send_out(0)
    for copy in sent[1]:
        copy.wait_recv()
    lax.fori_loop(0, 2, functools.partial(precondition, 1), 0)

    tile = (8, 128)
    row = lax.broadcasted_iota(jnp.int32, tile, 0)
    lane = lax.broadcasted_iota(jnp.int32, tile, 1)
    local = jnp.zeros(tile, F32)
    for j in range(2):
        block_at = source_ref[mine * 2 + j]
        param = param_ref[shard * nblk + jnp.minimum(block_at, nblk - 1)]
        param = jnp.where(block_at < nblk, param, -1)
        sums = jnp.where(row == 0, jnp.sum(acc[j, 0]), jnp.sum(acc[j, 1]))
        local = local + jnp.where((lane == param) & (row < 2), sums, 0.0)
    norm_ref[...] = local

    first = []
    for dy, dx, dc in OFFSETS:
        q = flat(y + dy, x + dx, c + dc)
        first.append(copies.start(norm_ref, norms.at[mine], {"dp": q}))
    send_out(1)
    norms[mine] = norm_ref[...]
    slots[mine] = direct[:, c, y, x]
    for load in states[3:5]:
        load.wait()

    def gram(i, carry):
        j, r = i // 4, i % 4
        at = pl.ds(pl.multiple_of(r * step, step), step)
        left = lax.dot_general(
            strip_of(j, r), whole(j), (((1,), (1,)), ((), ())), preferred_element_type=F32
        )
        nl_ref[j, at] = DECAY * nl_ref[j, at] + (1.0 - DECAY) * left
        columns_of = held[j, :, :, :, :, at].reshape(block, step)
        right = lax.dot_general(
            columns_of, whole(j), (((0,), (0,)), ((), ())), preferred_element_type=F32
        )
        nr_ref[j, at] = DECAY * nr_ref[j, at] + (1.0 - DECAY) * right
        return carry

    lax.fori_loop(0, 2, gram, 0)
    for copy in first:
        copy.wait_recv()
    total = norms[0]
    for i in range(1, norms.shape[0]):
        total = total + norms[i]
    group[...] = total
    third = [
        copies.start(group, columns.at[shard], {"shard": (shard + k) % n_shard})
        for k in range(1, n_shard)
    ]
    columns[shard] = total

    lax.fori_loop(2, 8, gram, 0)

    for copy in third:
        copy.wait_recv()
    total = columns[0]
    for i in range(1, n_shard):
        total = total + columns[i]
    ratio = jnp.sqrt((total[0:1] + TINY) / (total[1:2] + TINY))
    for copy in second:
        copy.wait_recv()
    for b in range(nblk):
        place = places[b]
        param = param_ref[shard * nblk + b]
        scale = jnp.sum(jnp.where(lane[0:1] == param, ratio, 0.0), axis=1, keepdims=True)
        out_ref[b, c, y, x] = (scale * slots[place // 2, place % 2].astype(F32)).astype(BF)

    arrivals = []

    def pass_on(where, *index):
        part = out_ref.at[index]
        return copies.start(part, part, where)

    def across_cores(*index):
        arrivals.append(pass_on(to_core, *index))

    xa = pass_on(to_x, A, c, y, x)
    b_near = [pass_on(to_up, B, c, y, x), pass_on(to_down, B, c, y, x)]
    xb = [pass_on(to_x, B, c, y, x)]
    a_near = [pass_on(to_up, A, c, y, x), pass_on(to_down, A, c, y, x)]
    across_cores(ALL, c, y, x)

    b_near[0].wait_recv()
    b_far = [pass_on(to_up, B, c, down, x, H[0])]
    xb.append(pass_on(to_x, B, c, down, x))
    b_near[1].wait_recv()
    b_far.append(pass_on(to_down, B, c, up, x, H[1]))
    xb.append(pass_on(to_x, B, c, up, x))
    across_cores(B, c, down, x)
    across_cores(B, c, up, x)

    xa.wait_recv()
    a_next = [pass_on(to_up, A, c, y, ox), pass_on(to_down, A, c, y, ox)]
    across_cores(A, c, y, ox)

    a_near[0].wait_recv()
    a_far = [pass_on(to_up, A, c, down, x, H[0])]
    across_cores(A, c, down, x)
    a_near[1].wait_recv()
    a_far.append(pass_on(to_down, A, c, up, x, H[1]))
    across_cores(A, c, up, x)

    b_far[0].wait_recv()
    b_far[1].wait_recv()
    xb.append(pass_on(to_x, B, c, across, x))
    across_cores(B, c, across, x)

    a_next[0].wait_recv()
    a_far.append(pass_on(to_up, A, c, down, ox, H[0]))
    across_cores(A, c, down, ox)
    a_next[1].wait_recv()
    a_far.append(pass_on(to_down, A, c, up, ox, H[1]))
    across_cores(A, c, up, ox)

    for i, chunk in enumerate((y, down, up)):
        xb[i].wait_recv()
        across_cores(B, c, chunk, ox)
    a_far[0].wait_recv()
    a_far[1].wait_recv()
    across_cores(A, c, across, x)
    a_far[2].wait_recv()
    a_far[3].wait_recv()
    across_cores(A, c, across, ox)
    xb[3].wait_recv()
    across_cores(B, c, across, ox)
    for copy in arrivals:
        copy.wait_recv()
    copies.finish()


def flush_kernel(*refs):
    count = len(refs) // 2
    sem = refs[-1]
    copies = [
        pltpu.make_async_copy(refs[i], refs[count + i], sem.at[i]) for i in range(count)
    ]
    for copy in copies:
        copy.start()
    for copy in copies:
        copy.wait()


def flush(*arrays):
    return pl.pallas_call(
        flush_kernel,
        out_shape=tuple(jax.ShapeDtypeStruct(a.shape, a.dtype) for a in arrays),
        in_specs=[pl.BlockSpec(memory_space=pltpu.VMEM)] * len(arrays),
        out_specs=tuple(pl.BlockSpec(memory_space=pltpu.HBM) for _ in arrays),
        scratch_shapes=[pltpu.SemaphoreType.DMA((len(arrays),))],
        compiler_params=pltpu.CompilerParams(vmem_limit_bytes=GRANT),
        name="flush",
    )(*arrays)


def on_device(gradients, owners, block_param, left_stat, right_stat, moment, left_root, right_root):
    _, nblk, block, width = gradients.shape
    n_shard = lax.axis_size("shard")
    n_dev = NY * NX * NC
    rows = block // n_dev
    na_blk = (nblk + 1) // 2
    nb_blk = nblk - na_blk
    n_copies = 23 + 5 * len(OFFSETS) + n_shard - 1 + 17 + 15
    state = jax.ShapeDtypeStruct((2, block, width), F32)
    hbm = pl.BlockSpec(memory_space=pltpu.HBM)
    vmem = pl.BlockSpec(memory_space=pltpu.VMEM)
    slot_rows = (2, NC, NY, NX, rows, width)
    new_left, new_right, new_moment, update = pl.pallas_call(
        functools.partial(step_kernel, nblk, na_blk, n_shard),
        out_shape=(
            state, state, state,
            jax.ShapeDtypeStruct((nblk, NC, NY, NX, rows, width), BF),
        ),
        in_specs=[hbm] * 8,
        out_specs=(vmem, vmem, vmem, vmem),
        scratch_shapes=[
            pltpu.VMEM((nblk, NY, NX, rows, width), BF),
            pltpu.VMEM((nblk, NC, NY, NX, rows, width), BF),
            pltpu.VMEM((nblk, NY, NX, rows, width), BF),
            pltpu.VMEM((2, na_blk, rows, width), BF),
            pltpu.VMEM((nb_blk, NY, rows, width), BF),
            pltpu.VMEM((2, 2, na_blk, rows, width), BF),
            pltpu.VMEM((na_blk, rows, width), BF),
            pltpu.VMEM((2, nb_blk, rows // 2, width), BF),
            pltpu.VMEM((2, 2, nb_blk, rows // 2, width), BF),
            pltpu.VMEM((nblk + 1, rows, width), BF),
            pltpu.VMEM((len(OFFSETS), 2, rows, width), BF),
            pltpu.VMEM(slot_rows, BF),
            pltpu.VMEM((2, block, width), BF),
            pltpu.VMEM((2, block, width), BF),
            pltpu.VMEM(slot_rows, BF),
            pltpu.VMEM((2, 2, 8, width), F32),
            pltpu.VMEM((8, 128), F32),
            pltpu.VMEM((n_dev, 2, rows, width), BF),
            pltpu.VMEM((n_dev, 8, 128), F32),
            pltpu.VMEM((8, 128), F32),
            pltpu.VMEM((n_shard, 8, 128), F32),
            pltpu.SMEM((2 * n_dev,), jnp.int32),
            pltpu.SMEM(owners.shape, jnp.int32),
            pltpu.SMEM(block_param.shape, jnp.int32),
            pltpu.SemaphoreType.DMA((6, 2)),
            pltpu.SemaphoreType.DMA((7,)),
            pltpu.SemaphoreType.DMA((n_copies,)),
            pltpu.SemaphoreType.DMA((n_copies,)),
        ],
        compiler_params=pltpu.CompilerParams(
            collective_id=0, has_side_effects=True, vmem_limit_bytes=GRANT
        ),
        name="shampoo_step",
    )(
        *(
            pltpu.with_memory_space_constraint(array, pltpu.HBM)
            for array in (
                owners, block_param,
                gradients.reshape(nblk, NC, NY, NX, rows, width),
                left_stat[:, 0], right_stat[:, 0], moment[:, 0], left_root[:, 0], right_root[:, 0],
            )
        ),
    )
    new_left, new_right, new_moment, update = flush(new_left, new_right, new_moment, update)
    return (
        new_left[:, None], new_right[:, None], new_moment[:, None],
        update.reshape(nblk, block, width),
    )


def solution(mesh):
    state = P("dp", "shard", None, None)
    return jax.shard_map(
        on_device,
        mesh=mesh,
        in_specs=(state, P("shard", None), P(), state, state, state, state, state),
        out_specs=(state, state, state, P("shard", None, None)),
        check_vma=False,
    )
```

```python
import functools

import jax
import jax.numpy as jnp
from jax import lax
from jax.experimental import pallas as pl
from jax.experimental.pallas import tpu as pltpu
from jax.sharding import PartitionSpec as P

DECAY = 0.95
TINY = 1e-06
NY, NX, NC = 4, 2, 2
GRANT = 30 << 20
BF = jnp.bfloat16
F32 = jnp.float32


def position():
    d = lax.axis_index("dp")
    return d // 4, (d // 2) % 2, d % 2


def flat(y, x, c):
    return (y % NY) * 4 + (x % NX) * 2 + c % NC


OFFSETS = [
    (dy, dx, dc)
    for dy in (1, 3, 2, 0)
    for dx in (1, 0)
    for dc in (0, 1)
    if (dy, dx, dc) != (0, 0, 0)
]


def slot_places(owner_ref, nblk):
    owners = [owner_ref[0, b] for b in range(nblk)]
    places = []
    for b in range(nblk):
        place = owners[b] * 2
        for other in range(b):
            place = place + jnp.where(owners[other] == owners[b], 1, 0)
        places.append(place)
    return places


class Copies:
    def __init__(self, send, recv):
        self.send, self.recv, self.count, self.all = send, recv, 0, []

    def start(self, src, dst, where):
        i = self.count
        self.count += 1
        copy = pltpu.make_async_remote_copy(
            src_ref=src,
            dst_ref=dst,
            send_sem=self.send.at[i],
            recv_sem=self.recv.at[i],
            device_id=where,
            device_id_type=pl.DeviceIdType.MESH,
        )
        copy.start()
        self.all.append(copy)
        return copy

    def finish(self):
        for copy in self.all:
            copy.wait_send()


def add_blocks(count, out, first, second):
    def body(b, carry):
        out[b] = first[b] + second[b]
        return carry

    lax.fori_loop(0, count, body, 0)


def add_many(count, out, *terms):
    def body(b, carry):
        total = terms[0][b].astype(F32)
        for term in terms[1:]:
            total = total + term[b].astype(F32)
        out[b] = total.astype(BF)
        return carry

    lax.fori_loop(0, count, body, 0)


def step_kernel(
    nblk, na_blk, n_shard, owner_hbm, param_hbm, grad_ref, lstat_hbm, rstat_hbm, moment_hbm,
    lroot_hbm, rroot_hbm, nl_ref, nr_ref, nm_ref, out_ref,
    loc, grad, rem, far_a, mid_b, near_a, mid_a, far_b, near_b, share, stage,
    held, lroot, rroot, direct, acc, norm_ref, slots, norms, group, columns,
    source_ref, owner_ref, param_ref, local_sem, state_sem, send_sem, recv_sem,
):
    y, x, c = position()
    mine = flat(y, x, c)
    shard = lax.axis_index("shard")
    nb_blk = nblk - na_blk
    rows = share.shape[1]
    half = rows // 2
    ox, oc = 1 - x, 1 - c
    up, down, across = (y + 1) % NY, (y + 3) % NY, (y + 2) % NY
    A = pl.ds(0, na_blk)
    B = pl.ds(na_blk, nb_blk)
    ALL = pl.ds(0, nblk)
    H = (pl.ds(0, half), pl.ds(half, half))

    def gpart(which, core, buf=grad):
        return [
            buf.at[A, core, across],
            buf.at[B, core, :, ox],
            buf.at[A, core, up],
            buf.at[A, core, down],
            buf.at[B, core, :, x],
            buf.at[A, core, y],
        ][which]

    def vpart(buf, which):
        return [
            buf.at[A, across],
            buf.at[B, :, ox],
            buf.at[A, up],
            buf.at[A, down],
            buf.at[B, :, x],
            buf.at[A, y],
        ][which]

    loads = {}
    for i in range(6):
        for own, core in enumerate((oc, c)):
            load = pltpu.make_async_copy(
                gpart(i, core, grad_ref), gpart(i, core), local_sem.at[i, own]
            )
            load.start()
            loads[i, own] = load
    states = [
        pltpu.make_async_copy(src, dst, state_sem.at[i])
        for i, (src, dst) in enumerate((
            (lroot_hbm, lroot), (rroot_hbm, rroot), (moment_hbm, nm_ref),
            (lstat_hbm, nl_ref), (rstat_hbm, nr_ref),
            (owner_hbm, owner_ref), (param_hbm, param_ref),
        ))
    ]

    barrier = pltpu.get_barrier_semaphore()
    for dy, dx, dc in OFFSETS:
        pl.semaphore_signal(
            barrier, inc=1, device_id={"dp": flat(y + dy, x + dx, c + dc)},
            device_id_type=pl.DeviceIdType.MESH,
        )
    for k in range(1, n_shard):
        pl.semaphore_signal(
            barrier, inc=1, device_id={"shard": (shard + k) % n_shard},
            device_id_type=pl.DeviceIdType.MESH,
        )
    pl.semaphore_wait(barrier, len(OFFSETS) + n_shard - 1)

    to_core = {"dp": flat(y, x, oc)}
    to_x = {"dp": flat(y, ox, c)}
    to_up = {"dp": flat(up, x, c)}
    to_down = {"dp": flat(down, x, c)}
    copies = Copies(send_sem, recv_sem)
    pair = []
    for i in range(6):
        loads[i, 0].wait()
        pair.append(copies.start(gpart(i, oc), vpart(rem, i), to_core))

    def pair_sum(i):
        loads[i, 1].wait()
        pair[i].wait_recv()
        out, mine, other = vpart(loc, i), gpart(i, c), vpart(rem, i)
        inner = mine.shape[1]
        for j in range(inner):
            add_blocks(out.shape[0], out.at[:, j], mine.at[:, j], other.at[:, j])

    for load in states:
        load.start()
    pair_sum(0)
    fa = [
        copies.start(loc.at[A, across, 0], far_a.at[0], to_up),
        copies.start(loc.at[A, across, 1], far_a.at[1], to_down),
    ]
    pair_sum(1)
    mb = [
        copies.start(loc.at[B, chunk, ox], mid_b.at[:, chunk], to_x)
        for chunk in (across, up, down, y)
    ]
    pair_sum(2)
    n_a = {(0, 1): copies.start(loc.at[A, up, 1], near_a.at[0, 1], to_up)}
    pair_sum(3)
    n_a[1, 0] = copies.start(loc.at[A, down, 0], near_a.at[1, 0], to_down)
    pair_sum(4)
    pair_sum(5)

    for load in states[5:]:
        load.wait()
    places = slot_places(owner_ref, nblk)

    def find(slot, carry):
        block = nblk
        for b in range(nblk):
            block = jnp.where(places[b] == slot, b, block)
        source_ref[slot] = block
        return carry

    lax.fori_loop(0, 2 * NY * NX * NC, find, 0)

    fa[0].wait_recv()
    add_blocks(na_blk, loc.at[A, up, 0], loc.at[A, up, 0], far_a.at[0])
    n_a[0, 0] = copies.start(loc.at[A, up, 0], near_a.at[0, 0], to_up)
    fa[1].wait_recv()
    add_blocks(na_blk, loc.at[A, down, 1], loc.at[A, down, 1], far_a.at[1])
    n_a[1, 1] = copies.start(loc.at[A, down, 1], near_a.at[1, 1], to_down)

    def middle(i, chunk):
        mb[i].wait_recv()
        add_blocks(nb_blk, loc.at[B, chunk, x], loc.at[B, chunk, x], mid_b.at[:, chunk])

    middle(0, across)
    fb = [
        copies.start(loc.at[B, across, x, H[0]], far_b.at[0], to_up),
        copies.start(loc.at[B, across, x, H[1]], far_b.at[1], to_down),
    ]
    middle(1, up)
    n_b = {(0, 1): copies.start(loc.at[B, up, x, H[1]], near_b.at[0, 1], to_up)}
    middle(2, down)
    n_b[1, 0] = copies.start(loc.at[B, down, x, H[0]], near_b.at[1, 0], to_down)

    for key in ((0, 1), (1, 0), (0, 0), (1, 1)):
        n_a[key].wait_recv()
    add_many(na_blk, loc.at[A, y, ox], loc.at[A, y, ox], near_a.at[0, ox], near_a.at[1, ox])
    ma = copies.start(loc.at[A, y, ox], mid_a, to_x)

    fb[0].wait_recv()
    add_blocks(nb_blk, loc.at[B, up, x, H[0]], loc.at[B, up, x, H[0]], far_b.at[0])
    n_b[0, 0] = copies.start(loc.at[B, up, x, H[0]], near_b.at[0, 0], to_up)
    fb[1].wait_recv()
    add_blocks(nb_blk, loc.at[B, down, x, H[1]], loc.at[B, down, x, H[1]], far_b.at[1])
    n_b[1, 1] = copies.start(loc.at[B, down, x, H[1]], near_b.at[1, 1], to_down)

    share[nblk] = jnp.zeros(share.shape[1:], BF)
    ma.wait_recv()
    add_many(
        na_blk, share.at[A], loc.at[A, y, x], near_a.at[0, x], near_a.at[1, x], mid_a
    )
    mb[3].wait_recv()
    for key in ((0, 1), (1, 0), (0, 0), (1, 1)):
        n_b[key].wait_recv()
    for h in range(2):
        add_many(
            nb_blk, share.at[B, H[h]], loc.at[B, y, x, H[h]], mid_b.at[:, y, H[h]],
            near_b.at[0, h], near_b.at[1, h],
        )

    sent = ([], [])
    for j in range(2):
        for k, (dy, dx, dc) in enumerate(OFFSETS):
            q = flat(y + dy, x + dx, c + dc)
            stage[k, j] = share[source_ref[q * 2 + j]]
            sent[j].append(copies.start(stage.at[k, j], held.at[j, c, y, x], {"dp": q}))
        held[j, c, y, x] = share[source_ref[mine * 2 + j]]
    for load in states[:3]:
        load.wait()
    step = 2 * NX * rows
    width = held.shape[-1]
    block = 4 * step

    def whole(j):
        return held[j].reshape(block, width)

    def strip_of(j, r):
        return held[j, r // 2, pl.ds(2 * (r % 2), 2)].reshape(step, width)

    acc[...] = jnp.zeros_like(acc)

    def precondition(j, r, carry):
        tall = 2 * step
        at = pl.ds(pl.multiple_of(r * tall, tall), tall)
        left = jnp.dot(lroot[j, at], whole(j), preferred_element_type=F32)
        high = left.astype(BF)
        low = (left - high.astype(F32)).astype(BF)
        direction = jnp.dot(high, rroot[j], preferred_element_type=F32)
        direction += jnp.dot(low, rroot[j], preferred_element_type=F32)
        direct[j, r] = direction.astype(BF).reshape(NY, NX, rows, width)
        wide = held[j, r].reshape(tall, width).astype(F32)
        moment = DECAY * nm_ref[j, at] + (1.0 - DECAY) * (wide * wide)
        nm_ref[j, at] = moment
        adam = wide / (jnp.sqrt(moment) + TINY)
        acc[j, 0] += jnp.sum((adam * adam).reshape(tall // 8, 8, width), axis=0)
        acc[j, 1] += jnp.sum((direction * direction).reshape(tall // 8, 8, width), axis=0)
        return carry

    second = []

    def send_out(j):
        for dy, dx, dc in OFFSETS:
            qy, qx, qc = (y + dy) % NY, (x + dx) % NX, (c + dc) % NC
            second.append(
                copies.start(
                    direct.at[j, qc, qy, qx], slots.at[mine, j], {"dp": flat(qy, qx, qc)}
                )
            )

    for copy in sent[0]:
        copy.wait_recv()
    lax.fori_loop(0, 2, functools.partial(precondition, 0), 0)
    send_out(0)
    for copy in sent[1]:
        copy.wait_recv()
    lax.fori_loop(0, 2, functools.partial(precondition, 1), 0)

    tile = (8, 128)
    row = lax.broadcasted_iota(jnp.int32, tile, 0)
    lane = lax.broadcasted_iota(jnp.int32, tile, 1)
    local = jnp.zeros(tile, F32)
    for j in range(2):
        block_at = source_ref[mine * 2 + j]
        param = param_ref[shard * nblk + jnp.minimum(block_at, nblk - 1)]
        param = jnp.where(block_at < nblk, param, -1)
        sums = jnp.where(row == 0, jnp.sum(acc[j, 0]), jnp.sum(acc[j, 1]))
        local = local + jnp.where((lane == param) & (row < 2), sums, 0.0)
    norm_ref[...] = local

    first = []
    for dy, dx, dc in OFFSETS:
        q = flat(y + dy, x + dx, c + dc)
        first.append(copies.start(norm_ref, norms.at[mine], {"dp": q}))
    send_out(1)
    norms[mine] = norm_ref[...]
    slots[mine] = direct[:, c, y, x]
    for load in states[3:5]:
        load.wait()

    def gram(i, carry):
        j, r = i // 4, i % 4
        at = pl.ds(pl.multiple_of(r * step, step), step)
        left = lax.dot_general(
            strip_of(j, r), whole(j), (((1,), (1,)), ((), ())), preferred_element_type=F32
        )
        nl_ref[j, at] = DECAY * nl_ref[j, at] + (1.0 - DECAY) * left
        columns_of = held[j, :, :, :, :, at].reshape(block, step)
        right = lax.dot_general(
            columns_of, whole(j), (((0,), (0,)), ((), ())), preferred_element_type=F32
        )
        nr_ref[j, at] = DECAY * nr_ref[j, at] + (1.0 - DECAY) * right
        return carry

    lax.fori_loop(0, 2, gram, 0)
    for copy in first:
        copy.wait_recv()
    total = norms[0]
    for i in range(1, norms.shape[0]):
        total = total + norms[i]
    group[...] = total
    third = [
        copies.start(group, columns.at[shard], {"shard": (shard + k) % n_shard})
        for k in range(1, n_shard)
    ]
    columns[shard] = total

    lax.fori_loop(2, 8, gram, 0)

    for copy in third:
        copy.wait_recv()
    total = columns[0]
    for i in range(1, n_shard):
        total = total + columns[i]
    ratio = jnp.sqrt((total[0:1] + TINY) / (total[1:2] + TINY))
    for copy in second:
        copy.wait_recv()
    for b in range(nblk):
        place = places[b]
        param = param_ref[shard * nblk + b]
        scale = jnp.sum(jnp.where(lane[0:1] == param, ratio, 0.0), axis=1, keepdims=True)
        out_ref[b, c, y, x] = (scale * slots[place // 2, place % 2].astype(F32)).astype(BF)

    arrivals = []

    def pass_on(where, *index):
        part = out_ref.at[index]
        return copies.start(part, part, where)

    def across_cores(*index):
        arrivals.append(pass_on(to_core, *index))

    xa = pass_on(to_x, A, c, y, x)
    b_near = [pass_on(to_up, B, c, y, x), pass_on(to_down, B, c, y, x)]
    xb = [pass_on(to_x, B, c, y, x)]
    a_near = [pass_on(to_up, A, c, y, x), pass_on(to_down, A, c, y, x)]
    across_cores(ALL, c, y, x)

    b_near[0].wait_recv()
    b_far = [pass_on(to_up, B, c, down, x, H[0])]
    xb.append(pass_on(to_x, B, c, down, x))
    b_near[1].wait_recv()
    b_far.append(pass_on(to_down, B, c, up, x, H[1]))
    xb.append(pass_on(to_x, B, c, up, x))
    across_cores(B, c, down, x)
    across_cores(B, c, up, x)

    xa.wait_recv()
    a_next = [pass_on(to_up, A, c, y, ox), pass_on(to_down, A, c, y, ox)]
    across_cores(A, c, y, ox)

    a_near[0].wait_recv()
    a_far = [pass_on(to_up, A, c, down, x, H[0])]
    across_cores(A, c, down, x)
    a_near[1].wait_recv()
    a_far.append(pass_on(to_down, A, c, up, x, H[1]))
    across_cores(A, c, up, x)

    b_far[0].wait_recv()
    b_far[1].wait_recv()
    xb.append(pass_on(to_x, B, c, across, x))
    across_cores(B, c, across, x)

    a_next[0].wait_recv()
    a_far.append(pass_on(to_up, A, c, down, ox, H[0]))
    across_cores(A, c, down, ox)
    a_next[1].wait_recv()
    a_far.append(pass_on(to_down, A, c, up, ox, H[1]))
    across_cores(A, c, up, ox)

    for i, chunk in enumerate((y, down, up)):
        xb[i].wait_recv()
        across_cores(B, c, chunk, ox)
    a_far[0].wait_recv()
    a_far[1].wait_recv()
    across_cores(A, c, across, x)
    a_far[2].wait_recv()
    a_far[3].wait_recv()
    across_cores(A, c, across, ox)
    xb[3].wait_recv()
    across_cores(B, c, across, ox)
    for copy in arrivals:
        copy.wait_recv()
    copies.finish()


def flush_kernel(*refs):
    count = len(refs) // 2
    sem = refs[-1]
    copies = []
    for i in range(count):
        length = refs[i].shape[0]
        for part in range(length):
            copies.append(
                pltpu.make_async_copy(
                    refs[i].at[part], refs[count + i].at[part], sem.at[len(copies)]
                )
            )
    for copy in copies:
        copy.start()
    for copy in copies:
        copy.wait()


def flush(*arrays):
    return pl.pallas_call(
        flush_kernel,
        out_shape=tuple(jax.ShapeDtypeStruct(a.shape, a.dtype) for a in arrays),
        in_specs=[pl.BlockSpec(memory_space=pltpu.VMEM)] * len(arrays),
        out_specs=tuple(pl.BlockSpec(memory_space=pltpu.HBM) for _ in arrays),
        scratch_shapes=[pltpu.SemaphoreType.DMA((sum(a.shape[0] for a in arrays),))],
        compiler_params=pltpu.CompilerParams(vmem_limit_bytes=GRANT),
        name="flush",
    )(*arrays)


def on_device(gradients, owners, block_param, left_stat, right_stat, moment, left_root, right_root):
    _, nblk, block, width = gradients.shape
    n_shard = lax.axis_size("shard")
    n_dev = NY * NX * NC
    rows = block // n_dev
    na_blk = (nblk + 1) // 2
    nb_blk = nblk - na_blk
    n_copies = 23 + 5 * len(OFFSETS) + n_shard - 1 + 17 + 15
    state = jax.ShapeDtypeStruct((2, block, width), F32)
    hbm = pl.BlockSpec(memory_space=pltpu.HBM)
    vmem = pl.BlockSpec(memory_space=pltpu.VMEM)
    slot_rows = (2, NC, NY, NX, rows, width)
    new_left, new_right, new_moment, update = pl.pallas_call(
        functools.partial(step_kernel, nblk, na_blk, n_shard),
        out_shape=(
            state, state, state,
            jax.ShapeDtypeStruct((nblk, NC, NY, NX, rows, width), BF),
        ),
        in_specs=[hbm] * 8,
        out_specs=(vmem, vmem, vmem, vmem),
        scratch_shapes=[
            pltpu.VMEM((nblk, NY, NX, rows, width), BF),
            pltpu.VMEM((nblk, NC, NY, NX, rows, width), BF),
            pltpu.VMEM((nblk, NY, NX, rows, width), BF),
            pltpu.VMEM((2, na_blk, rows, width), BF),
            pltpu.VMEM((nb_blk, NY, rows, width), BF),
            pltpu.VMEM((2, 2, na_blk, rows, width), BF),
            pltpu.VMEM((na_blk, rows, width), BF),
            pltpu.VMEM((2, nb_blk, rows // 2, width), BF),
            pltpu.VMEM((2, 2, nb_blk, rows // 2, width), BF),
            pltpu.VMEM((nblk + 1, rows, width), BF),
            pltpu.VMEM((len(OFFSETS), 2, rows, width), BF),
            pltpu.VMEM(slot_rows, BF),
            pltpu.VMEM((2, block, width), BF),
            pltpu.VMEM((2, block, width), BF),
            pltpu.VMEM(slot_rows, BF),
            pltpu.VMEM((2, 2, 8, width), F32),
            pltpu.VMEM((8, 128), F32),
            pltpu.VMEM((n_dev, 2, rows, width), BF),
            pltpu.VMEM((n_dev, 8, 128), F32),
            pltpu.VMEM((8, 128), F32),
            pltpu.VMEM((n_shard, 8, 128), F32),
            pltpu.SMEM((2 * n_dev,), jnp.int32),
            pltpu.SMEM(owners.shape, jnp.int32),
            pltpu.SMEM(block_param.shape, jnp.int32),
            pltpu.SemaphoreType.DMA((6, 2)),
            pltpu.SemaphoreType.DMA((7,)),
            pltpu.SemaphoreType.DMA((n_copies,)),
            pltpu.SemaphoreType.DMA((n_copies,)),
        ],
        compiler_params=pltpu.CompilerParams(
            collective_id=0, has_side_effects=True, vmem_limit_bytes=GRANT
        ),
        name="shampoo_step",
    )(
        *(
            pltpu.with_memory_space_constraint(array, pltpu.HBM)
            for array in (
                owners, block_param,
                gradients.reshape(nblk, NC, NY, NX, rows, width),
                left_stat[:, 0], right_stat[:, 0], moment[:, 0], left_root[:, 0], right_root[:, 0],
            )
        ),
    )
    new_left, new_right, new_moment, update = flush(new_left, new_right, new_moment, update)
    return (
        new_left[:, None], new_right[:, None], new_moment[:, None],
        update.reshape(nblk, block, width),
    )


def solution(mesh):
    state = P("dp", "shard", None, None)
    return jax.shard_map(
        on_device,
        mesh=mesh,
        in_specs=(state, P("shard", None), P(), state, state, state, state, state),
        out_specs=(state, state, state, P("shard", None, None)),
        check_vma=False,
    )
```
